32 devices in a mesh: freq: 4 (over y, x), pts: 8 (over z, core).
Axes of the slice: x: 2, y: 2, z: 4, core: 2. Of those that a mesh axis runs over, the one named last changes fastest.
Arguments:
- data: float32 [2, 32, 64, 3, 8192], P(None, 'freq', None, None, 'pts'), may hold values from -180 to 180
- quad_weight: float32 [8192], P('pts'), may hold values from 0.2 to 5
- basis: float32 [2, 32, 64, 8], P(None, 'freq'), may hold values from -6 to 6
Outputs:
- basis_out: float32 [2, 32, 64, 8], P(None, 'freq')
- spectrum: float32 [32, 8], P('freq')
- modes: float32 [2, 32, 8, 3, 8192], P(None, 'freq', None, None, 'pts')
The draws below stay inside these ranges and needn't reach their ends.
All inputs are finite; a program needn't handle non-finite values.
Results may differ from the reference program's by a relative error of at most 0.0001.
Values sent between devices are 32-bit elements; how exact they have to be, the bound alone decides.
A program may use at most 128 MiB of HBM per device.

```python
import math
import jax
import jax.numpy as jnp
from jax import lax

BLOCKS = 64
RANK = 8
COMP = 3
ITERS = 4
FREQ_ALL = 32
NPTS = 8192


def draw_data(key, part):
    first, second = jax.random.split(key, 2)
    shape = (2, FREQ_ALL, BLOCKS, COMP, NPTS)
    ramp = 1.0 + 2.0 * jnp.arange(FREQ_ALL, dtype=jnp.float32) / max(FREQ_ALL - 1, 1)
    block_scale = jnp.exp(jax.random.uniform(second, (FREQ_ALL, BLOCKS), jnp.float32, 0.0, math.log(10.0)))
    values = jnp.clip(jax.random.normal(first, shape, jnp.float32), -6.0, 6.0)
    scaled = values * (ramp[:, None] * block_scale)[None, :, :, None, None]
    return scaled.astype(jnp.float32)


def level_of(key, dims, pieces, smallest, high):
    factor_of = 1.0
    for axis_at, parts in pieces:
        heights = jax.random.uniform(jax.random.fold_in(jax.random.fold_in(key, 6), axis_at), (parts,), jnp.float32, smallest / len(pieces), high / len(pieces))
        factor_of = factor_of * jnp.repeat(jnp.exp(heights), dims[axis_at] // parts).reshape((-1,) + (1,) * (len(dims) - 1 - axis_at))
    return factor_of


def scatter_about(stream_key, dims, deviation, limit, shards=(), kind=jnp.bfloat16):
    gain = level_of(stream_key, dims, shards, -0.22, 0.18) if shards else 1.0
    result = jax.random.normal(stream_key, dims, jnp.float32) * deviation * gain
    return jnp.minimum(jnp.maximum(result, -limit), limit).astype(kind)


def setup_inputs(seed: int = 0) -> dict:
    keys = jax.random.split(jax.random.key(seed), 4)
    data = draw_data(jax.random.fold_in(keys[3], 71), 0)
    quad_weight = jnp.clip(jnp.exp(math.log(5.0) - 3.218876 * jax.random.uniform(keys[1], (NPTS,), jnp.float32) ** level_of(keys[1], (NPTS,), ((0, 8),), -0.2, 0.2)), 0.2, 5.0)
    basis = scatter_about(keys[2], (2, FREQ_ALL, BLOCKS, RANK), 1.0, 6.0, ((1, 4),), jnp.float32)
    return dict(data=data, quad_weight=quad_weight, basis=basis)


def matmul_high(left, right):
    return jnp.matmul(left, right, precision=lax.Precision.HIGHEST)

def apply_gram(gram_real, gram_imag, vec_real, vec_imag):
    out_real = matmul_high(gram_real, vec_real) - matmul_high(gram_imag, vec_imag)
    out_imag = matmul_high(gram_real, vec_imag) + matmul_high(gram_imag, vec_real)
    return (out_real, out_imag)

def orthonormalize(z_real, z_imag):
    blocks = z_real.shape[-2]
    cols_real = []
    cols_imag = []
    for column in range(z_real.shape[-1]):
        cur_real = z_real[..., column]
        cur_imag = z_imag[..., column]
        for earlier in range(column):
            base_real = cols_real[earlier]
            base_imag = cols_imag[earlier]
            coef_real = lax.optimization_barrier(jnp.sum(base_real * cur_real + base_imag * cur_imag, axis=-1)) / blocks
            coef_imag = lax.optimization_barrier(jnp.sum(base_real * cur_imag - base_imag * cur_real, axis=-1)) / blocks
            cur_real = cur_real - (coef_real[..., None] * base_real - coef_imag[..., None] * base_imag)
            cur_imag = cur_imag - (coef_real[..., None] * base_imag + coef_imag[..., None] * base_real)
        factor = lax.rsqrt(lax.optimization_barrier(jnp.mean(cur_real * cur_real + cur_imag * cur_imag, axis=-1)) + 1e-06)
        cols_real.append(cur_real * factor[..., None])
        cols_imag.append(cur_imag * factor[..., None])
    return (jnp.stack(cols_real, axis=-1), jnp.stack(cols_imag, axis=-1))

def reference(data, quad_weight, basis):
    scaling = 1.0 / (COMP * NPTS)
    weights = jnp.tile(quad_weight, COMP)

    def one_freq(index):
        block = lax.dynamic_index_in_dim(data, index, 1, keepdims=False)
        samples = block.reshape(2, BLOCKS, COMP * NPTS)
        weighted = samples * weights[None, None, :]
        gram_real = (matmul_high(samples[0], weighted[0].T) + matmul_high(samples[1], weighted[1].T)) * scaling
        gram_imag = (matmul_high(samples[0], weighted[1].T) - matmul_high(samples[1], weighted[0].T)) * scaling
        start = lax.dynamic_index_in_dim(basis, index, 1, keepdims=False)
        vec_real = start[0]
        vec_imag = start[1]
        for step in range(ITERS):
            z_real, z_imag = apply_gram(gram_real, gram_imag, vec_real, vec_imag)
            vec_real, vec_imag = orthonormalize(z_real, z_imag)
        z_real, z_imag = apply_gram(gram_real, gram_imag, vec_real, vec_imag)
        rayleigh = lax.optimization_barrier(jnp.sum(vec_real * z_real + vec_imag * z_imag, axis=-2)) / BLOCKS
        proj_real = matmul_high(vec_real.T, samples[0]) - matmul_high(vec_imag.T, samples[1])
        proj_imag = matmul_high(vec_imag.T, samples[0]) + matmul_high(vec_real.T, samples[1])
        projected = jnp.stack([proj_real, proj_imag]) / BLOCKS
        trace_value = jnp.sum(jnp.diagonal(gram_real))
        return (jnp.stack([vec_real, vec_imag]), rayleigh, projected.reshape(2, RANK, COMP, NPTS), trace_value)
    bases, rayleigh, projected, traces = lax.map(one_freq, jnp.arange(FREQ_ALL, dtype=jnp.int32))
    total = jnp.sum(traces)
    spectrum = rayleigh * (FREQ_ALL * BLOCKS) / total
    return (jnp.moveaxis(bases, 0, 1), spectrum, jnp.moveaxis(projected, 0, 1))
```

```python
import functools

import jax
import jax.numpy as jnp
from jax import lax
from jax.experimental import pallas as pl
from jax.experimental.pallas import tpu as pltpu
from jax.sharding import PartitionSpec as P

ITERS = 4
EPS = 1e-06
MESH = pl.DeviceIdType.MESH


def partner(index, mask, size):
    if size & (size - 1):
        return lax.rem(index + mask, size)
    result, bit = 0, 1
    while bit < size:
        if isinstance(mask, int):
            one = lax.rem(lax.div(index, bit), 2)
            result = result + bit * (1 - one if mask & bit else one)
        else:
            one = lax.rem(lax.div(index, bit), 2)
            other = lax.rem(lax.div(mask, bit), 2)
            result = result + bit * (one + other - 2 * one * other)
        bit *= 2
    return result


def slot_of(source, target, size):
    return lax.rem(source - target - 1 + size, size)


def wait_bytes(ref, sem):
    pltpu.make_async_copy(ref, ref, sem).wait()


def project_one(vec, split, f, inverse, stage, at):
    rank, wide = vec.shape
    blocks = wide // 2
    lanes = lax.broadcasted_iota(jnp.int32, (1, wide), 1)
    high_minus = jnp.where(lanes < blocks, 1.0, -1.0).astype(jnp.float32)
    left = jnp.concatenate([high_minus * vec, pltpu.roll(vec, blocks, 1)], axis=0)
    high = left.astype(jnp.bfloat16)
    rest = (left - high.astype(jnp.float32)).astype(jnp.bfloat16)
    both = jnp.concatenate([high, high], axis=1)
    tail = jnp.concatenate([rest, jnp.zeros_like(rest)], axis=1)
    left = jnp.concatenate([both, tail], axis=0)
    for c in range(split.shape[1]):
        out = jnp.dot(left, split[f, c], preferred_element_type=jnp.float32)
        out = (out[: 2 * rank] + out[2 * rank :]) * inverse
        stage[at, 0, c] = out[:rank]
        stage[at, 1, c] = out[rank:]


def orthonormalize(z, turned, blocks, group):
    rank, wide = z.shape
    which = lax.broadcasted_iota(jnp.int32, (rank, wide), 0)
    for first in range(0, rank, group):
        rows = range(first, min(first + group, rank))
        real, imag = {}, {}
        for j in rows:
            real[j] = jnp.sum(z * z[j : j + 1], axis=1, keepdims=True)
            imag[j] = jnp.sum(z * turned[j : j + 1], axis=1, keepdims=True)
        for j in rows:
            real[j] = jnp.broadcast_to(real[j], z.shape) * (1.0 / blocks)
            imag[j] = jnp.broadcast_to(imag[j], z.shape) * (1.0 / blocks)
        for j in rows:
            square = jnp.maximum(real[j][j : j + 1], 0.0)
            factor = lax.rsqrt(square + EPS)
            gain = factor * factor
            gain = gain * (1.0 + EPS * gain)
            later = which > j
            along = jnp.where(later, real[j], 0.0)
            across = jnp.where(later, imag[j], 0.0)
            for k in rows:
                if k > j:
                    up = along[k : k + 1] * gain
                    side = across[k : k + 1] * gain
                    real[k] = real[k] - (up * along + side * across)
                    imag[k] = imag[k] - (up * across - side * along)
            unit = z[j : j + 1] * factor
            unit_turned = turned[j : j + 1] * factor
            along = along * factor
            across = across * factor
            z_next = z - (along * unit + across * unit_turned)
            turned = turned - (along * unit_turned - across * unit)
            z = jnp.where(which == j, unit, z_next)
    return z


def spod_kernel(
    scaling,
    freqs,
    peers,
    groups,
    early,
    data_ref,
    weight_hbm,
    basis_hbm,
    split,
    message_ref,
    scalar_ref,
    inverse_ref,
    stage,
    buf,
    weight_ref,
    basis_ref,
    raw,
    gram_out,
    gram_in,
    trace_out,
    trace_in,
    message,
    scalar_out,
    scalar_in,
    small_sem,
    load_sem,
    gram_sem,
    trace_sem,
    msg_send,
    msg_recv,
    scalar_sem,
):
    comps, blocks, points = buf.shape[2], buf.shape[3], buf.shape[4]
    rank = basis_ref.shape[1]
    wide = 2 * blocks
    half_rows = blocks // 2
    stride = peers // freqs
    me = lax.axis_index("pts")
    row = lax.axis_index("freq")
    mine = lax.div(me, stride)
    is_owner = lax.rem(me, stride) == 0
    hold = min(2, freqs - 1)
    f32 = jnp.float32

    def load(f):
        return pltpu.make_async_copy(data_ref.at[:, f], buf.at[f], load_sem.at[f])

    def order(i):
        return partner(mine, freqs - 1 - i, freqs)

    weight_load = pltpu.make_async_copy(weight_hbm, weight_ref, small_sem.at[0])
    basis_load = pltpu.make_async_copy(basis_hbm.at[:, mine], basis_ref, small_sem.at[1])
    weight_load.start()
    for i in range(freqs):
        load(order(i)).start()
    basis_load.start()

    barrier = pltpu.get_barrier_semaphore()
    for step in range(1, peers):
        pl.semaphore_signal(
            barrier, inc=1, device_id={"pts": lax.rem(me + step, peers)}, device_id_type=MESH
        )
    for step in range(1, groups):
        pl.semaphore_signal(
            barrier, inc=1, device_id={"freq": lax.rem(row + step, groups)}, device_id_type=MESH
        )

    lanes = lax.broadcasted_iota(jnp.int32, (1, wide), 1)
    low = lanes < blocks
    high_minus = jnp.where(low, 1.0, -1.0).astype(f32)
    raw[...] = jnp.zeros_like(raw)
    weight_load.wait()
    root = jnp.sqrt(weight_ref[...])
    inverse_ref[...] = (1.0 / blocks) / root

    rows_at = lax.broadcasted_iota(jnp.int32, (half_rows, wide), 0)
    cols_at = lax.broadcasted_iota(jnp.int32, (half_rows, wide), 1)
    diagonal = jnp.logical_or(cols_at == rows_at, cols_at == rows_at + blocks + half_rows)

    def local_gram(f):
        load(f).wait()
        total = jnp.zeros((2 * wide, wide), f32)
        for c in range(comps):
            for part in range(2):
                value = buf[f, part, c] * root
                high = value.astype(jnp.bfloat16)
                rest = (value - high.astype(f32)).astype(jnp.bfloat16)
                split[f, c, part * blocks : (part + 1) * blocks] = high
                split[f, c, wide + part * blocks : wide + (part + 1) * blocks] = rest
            total = total + lax.dot_general(
                split[f, c],
                split[f, c, :wide],
                (((1,), (1,)), ((), ())),
                preferred_element_type=f32,
            )
        raw[...] = 0.5 * total[:wide] + total[wide:]

    def pack(f):
        total = raw[...]
        both = total[:blocks] + high_minus * pltpu.roll(total[blocks:], blocks, 1)
        other = pltpu.roll(both, blocks, 1)
        minus = both - other
        flipped = jnp.concatenate([minus, minus], axis=0).T
        full = both + other + flipped[:blocks]
        folded = jnp.where(low, full[:half_rows], full[half_rows:])
        gram_out[f] = folded
        return jnp.where(diagonal, folded, 0.0)

    def gram_copy(f):
        target = f * stride
        return pltpu.make_async_remote_copy(
            src_ref=gram_out.at[f],
            dst_ref=gram_in.at[slot_of(me, target, peers)],
            send_sem=gram_sem.at[0],
            recv_sem=gram_sem.at[1],
            device_id={"pts": target},
            device_id_type=MESH,
        )

    def opening(i, trace):
        trace = trace + pack(order(jnp.maximum(i - 1, 0)))
        local_gram(order(i))
        return trace

    trace = lax.fori_loop(0, hold, opening, jnp.zeros((half_rows, wide), f32))
    pl.semaphore_wait(barrier, peers - 1 + groups - 1)
    for i in range(hold - 1):
        gram_copy(order(i)).start()

    def middle(i, trace):
        last = order(i - 1)
        trace = trace + pack(last)
        gram_copy(last).start()
        local_gram(order(i))
        return trace

    trace = lax.fori_loop(hold, freqs, middle, trace)
    trace = trace + pack(mine)
    if stride > 1:

        @pl.when(jnp.logical_not(is_owner))
        def _():
            gram_copy(mine).start()

    trace_row = jnp.sum(trace, axis=0, keepdims=True) * scaling
    trace_out[...] = trace_row

    def trace_copy(step):
        target = lax.rem(row + step, groups)
        return pltpu.make_async_remote_copy(
            src_ref=trace_out,
            dst_ref=trace_in.at[slot_of(row, target, groups)],
            send_sem=trace_sem.at[0],
            recv_sem=trace_sem.at[1],
            device_id={"freq": target},
            device_id_type=MESH,
        )

    for step in range(1, groups):
        trace_copy(step).start()

    def msg_copy(step):
        return pltpu.make_async_remote_copy(
            src_ref=message.at[mine],
            dst_ref=message.at[mine],
            send_sem=msg_send.at[0],
            recv_sem=msg_recv.at[mine],
            device_id={"pts": partner(me, step, peers)},
            device_id_type=MESH,
        )

    def scalar_copy(step):
        target = partner(me, step, peers)
        return pltpu.make_async_remote_copy(
            src_ref=scalar_out,
            dst_ref=scalar_in.at[slot_of(me, target, peers)],
            send_sem=scalar_sem.at[0],
            recv_sem=scalar_sem.at[1],
            device_id={"pts": target},
            device_id_type=MESH,
        )

    basis_load.wait()
    scalar_out[...] = jnp.zeros_like(scalar_out)

    @pl.when(is_owner)
    def _():
        wait_bytes(gram_in.at[pl.ds(0, peers - 1)], gram_sem.at[1])
        total = gram_out[mine]
        for k in range(peers - 1):
            total = total + gram_in[k]
        total = total * (0.5 * scaling)
        swapped = pltpu.roll(total, blocks, 1)
        full = jnp.concatenate(
            [jnp.where(low, total, swapped), jnp.where(low, swapped, total)], axis=0
        )
        full = jnp.concatenate([full, full], axis=0)
        flipped = full.T
        real = full + flipped
        imag = full - flipped
        top = lax.broadcasted_iota(jnp.int32, (wide, wide), 0) < blocks
        left = lax.broadcasted_iota(jnp.int32, (wide, wide), 1) < blocks
        same = top == left
        matrix = jnp.where(same, real, jnp.where(top, -imag, imag))
        turning = jnp.where(same, imag, jnp.where(top, real, -real))
        right = jnp.concatenate([matrix, turning], axis=1)

        def rounded(x):
            return x.astype(jnp.bfloat16).astype(f32)

        right_high = rounded(right)
        right_rest = right - right_high
        right_mid = rounded(right_rest)
        right_low = rounded(right_rest - right_mid)
        right_pair = jnp.concatenate([right_high, right_mid], axis=0)

        def apply(vec):
            high = rounded(vec)
            rest = vec - high
            mid = rounded(rest)
            tail = rounded(rest - mid)
            rows = jnp.concatenate(
                [
                    jnp.concatenate([high, high], axis=1),
                    jnp.concatenate([mid, mid], axis=1),
                    jnp.concatenate([tail, jnp.zeros_like(tail)], axis=1),
                ],
                axis=0,
            )
            out = jnp.dot(rows, right_pair, preferred_element_type=f32)
            small = jnp.dot(high, right_low, preferred_element_type=f32)
            out = out[:rank] + (out[rank : 2 * rank] + (out[2 * rank :] + small))
            return out[:, :wide], out[:, wide:]

        vec = jnp.concatenate([basis_ref[0], basis_ref[1]], axis=1)
        for step in range(ITERS):
            z, turned = apply(vec)
            vec = orthonormalize(z, turned, blocks, rank if step < ITERS - 1 else rank // 2)
        message[mine] = vec
        for step in range(peers - 1, 0, -1):
            msg_copy(step).start()
        energy = jnp.sum(vec * apply(vec)[0], axis=1, keepdims=True) * (1.0 / blocks)
        which = lax.broadcasted_iota(jnp.int32, (rank, wide), 0)
        columns = lax.broadcasted_iota(jnp.int32, (rank, wide), 1)
        scalar_out[0:1] = jnp.sum(jnp.where(which == columns, energy, 0.0), axis=0, keepdims=True)

    wait_bytes(trace_in.at[pl.ds(0, groups - 1)], trace_sem.at[1])
    group_trace = trace_out[...]
    for k in range(groups - 1):
        group_trace = group_trace + trace_in[k]
    scalar_out[1:2] = group_trace
    for step in range(peers - 1, 0, -1):
        scalar_copy(step).start()

    inverse = inverse_ref[...]

    def arrive(i):
        f = partner(mine, i, freqs)
        if stride > 1:

            @pl.when(jnp.logical_or(i > 0, jnp.logical_not(is_owner)))
            def _():
                wait_bytes(message.at[f], msg_recv.at[f])
        else:

            @pl.when(i > 0)
            def _():
                wait_bytes(message.at[f], msg_recv.at[f])

        return f

    def ahead(i, carry):
        f = arrive(i)
        project_one(message[f], split, f, inverse, stage, f)
        return carry

    lax.fori_loop(0, early, ahead, 0)

    def others(i, carry):
        arrive(i)
        return carry

    lax.fori_loop(early, freqs, others, 0)
    wait_bytes(scalar_in.at[pl.ds(0, peers - 1)], scalar_sem.at[1])
    message_ref[...] = message[...]
    scalar_ref[pl.ds(0, peers - 1)] = scalar_in[pl.ds(0, peers - 1)]
    scalar_ref[peers - 1] = scalar_out[...]

    if stride > 1:

        @pl.when(jnp.logical_not(is_owner))
        def _():
            wait_bytes(gram_out, gram_sem.at[0])

        @pl.when(is_owner)
        def _():
            wait_bytes(gram_out.at[pl.ds(0, freqs - 1)], gram_sem.at[0])
    else:
        wait_bytes(gram_out.at[pl.ds(0, freqs - 1)], gram_sem.at[0])

    wait_bytes(trace_in.at[pl.ds(0, groups - 1)], trace_sem.at[0])
    wait_bytes(scalar_in.at[pl.ds(0, peers - 1)], scalar_sem.at[0])

    @pl.when(is_owner)
    def _():
        wait_bytes(gram_in.at[pl.ds(0, peers - 1), pl.ds(0, rank)], msg_send.at[0])


def project_kernel(
    count,
    freqs,
    peers,
    early,
    inverse_ref,
    split,
    message,
    scalar,
    stage,
    basis_out,
    spectrum_out,
    modes_out,
    late_stage,
    basis_stage,
    spectrum_stage,
    store_sem,
):
    wide = message.shape[2]
    blocks = wide // 2
    rank = message.shape[1]
    stride = peers // freqs
    me = lax.axis_index("pts")
    mine = lax.div(me, stride)

    def start(i, carry):
        f = partner(mine, i, freqs)
        pltpu.make_async_copy(stage.at[f], modes_out.at[:, f], store_sem.at[0]).start()
        return carry

    lax.fori_loop(0, early, start, 0)

    def late(i, carry):
        f = partner(mine, i, freqs)
        project_one(message[f], split, f, inverse_ref[...], late_stage, i - early)
        pltpu.make_async_copy(
            late_stage.at[i - early], modes_out.at[:, f], store_sem.at[0]
        ).start()
        return carry

    lax.fori_loop(early, freqs, late, 0)

    vecs = message[...]
    turned = pltpu.roll(vecs, blocks, 2)
    basis_stage[0] = vecs[:, :, :blocks]
    basis_stage[1] = turned[:, :, :blocks]
    basis_store = pltpu.make_async_copy(basis_stage, basis_out, store_sem.at[1])
    basis_store.start()

    energies = []
    for f in range(freqs):
        energies.append(scalar[slot_of(f * stride, me, peers), 0:1])
    overall = jnp.zeros((1, wide), jnp.float32)
    for k in range(peers):
        overall = overall + scalar[k, 1:2]
    overall = jnp.sum(overall, axis=1, keepdims=True)
    spectrum = jnp.concatenate(energies, axis=0) * count / overall
    spectrum_stage[...] = spectrum[:, :rank]
    spectrum_store = pltpu.make_async_copy(spectrum_stage, spectrum_out, store_sem.at[2])
    spectrum_store.start()

    wait_bytes(modes_out, store_sem.at[0])
    basis_store.wait()
    spectrum_store.wait()


def per_device(peers, groups, data, quad_weight, basis):
    _, freqs, blocks, comps, points = data.shape
    rank = basis.shape[-1]
    assert peers % freqs == 0 and freqs > 2
    scaling = 1.0 / (comps * points * peers)
    wide = 2 * blocks
    early = freqs - 2
    vmem = pl.BlockSpec(memory_space=pltpu.VMEM)
    anywhere = pl.BlockSpec(memory_space=pl.ANY)
    f32 = jnp.float32
    weight = quad_weight.reshape(1, points)
    hbm = pl.BlockSpec(memory_space=pltpu.HBM)
    in_hbm = functools.partial(pltpu.with_memory_space_constraint, memory_space=pltpu.HBM)
    split, message, scalar, inverse, stage = pl.pallas_call(
        functools.partial(spod_kernel, scaling, freqs, peers, groups, early),
        out_shape=(
            pltpu.VMEM((freqs, comps, 2 * wide, points), jnp.bfloat16),
            pltpu.VMEM((freqs, rank, wide), f32),
            pltpu.VMEM((peers, 2, wide), f32),
            pltpu.VMEM((1, points), f32),
            pltpu.VMEM((freqs, 2, comps, rank, points), f32),
        ),
        in_specs=[hbm, hbm, hbm],
        out_specs=(vmem, vmem, vmem, vmem, vmem),
        scratch_shapes=[
            pltpu.VMEM((freqs, 2, comps, blocks, points), f32),
            pltpu.VMEM((1, points), f32),
            pltpu.VMEM((2, rank, blocks), f32),
            pltpu.VMEM((wide, wide), f32),
            pltpu.VMEM((freqs, blocks // 2, wide), f32),
            pltpu.VMEM((peers, blocks // 2, wide), f32),
            pltpu.VMEM((1, wide), f32),
            pltpu.VMEM((groups, 1, wide), f32),
            pltpu.VMEM((freqs, rank, wide), f32),
            pltpu.VMEM((2, wide), f32),
            pltpu.VMEM((peers, 2, wide), f32),
            pltpu.SemaphoreType.DMA((2,)),
            pltpu.SemaphoreType.DMA((freqs,)),
            pltpu.SemaphoreType.DMA((2,)),
            pltpu.SemaphoreType.DMA((2,)),
            pltpu.SemaphoreType.DMA((1,)),
            pltpu.SemaphoreType.DMA((freqs,)),
            pltpu.SemaphoreType.DMA((2,)),
        ],
        compiler_params=pltpu.CompilerParams(
            collective_id=0, has_side_effects=True, vmem_limit_bytes=44 * 1024 * 1024
        ),
        name="spod",
    )(
        in_hbm(data.transpose(0, 1, 3, 2, 4)),
        in_hbm(weight),
        in_hbm(basis.transpose(0, 1, 3, 2)),
    )
    basis_t, spectrum, modes_t = pl.pallas_call(
        functools.partial(project_kernel, freqs * groups * blocks, freqs, peers, early),
        out_shape=(
            jax.ShapeDtypeStruct((2, freqs, rank, blocks), f32),
            jax.ShapeDtypeStruct((freqs, rank), f32),
            jax.ShapeDtypeStruct((2, freqs, comps, rank, points), f32),
        ),
        in_specs=[vmem, vmem, vmem, vmem, vmem],
        out_specs=(anywhere, anywhere, anywhere),
        scratch_shapes=[
            pltpu.VMEM((freqs - early, 2, comps, rank, points), f32),
            pltpu.VMEM((2, freqs, rank, blocks), f32),
            pltpu.VMEM((freqs, rank), f32),
            pltpu.SemaphoreType.DMA((3,)),
        ],
        compiler_params=pltpu.CompilerParams(vmem_limit_bytes=20 * 1024 * 1024),
        name="project",
    )(inverse, split, message, scalar, stage)
    return (
        basis_t.transpose(0, 1, 3, 2),
        spectrum,
        modes_t.transpose(0, 1, 3, 2, 4),
    )


def solution(mesh):
    in_specs = (P(None, "freq", None, None, "pts"), P("pts"), P(None, "freq", None, None))
    out_specs = (P(None, "freq", None, None), P("freq", None), P(None, "freq", None, None, "pts"))
    body = functools.partial(per_device, mesh.shape["pts"], mesh.shape["freq"])
    return jax.shard_map(
        body, mesh=mesh, in_specs=in_specs, out_specs=out_specs, check_vma=False
    )
```

```python
import functools

import jax
import jax.numpy as jnp
from jax import lax
from jax.experimental import pallas as pl
from jax.experimental.pallas import tpu as pltpu
from jax.sharding import PartitionSpec as P

ITERS = 4
EPS = 1e-06
HOLD = 2
LATE = 4
MESH = pl.DeviceIdType.MESH


def partner(index, mask, size):
    if size & (size - 1):
        return lax.rem(index + mask, size)
    result, bit = 0, 1
    while bit < size:
        if isinstance(mask, int):
            one = lax.rem(lax.div(index, bit), 2)
            result = result + bit * (1 - one if mask & bit else one)
        else:
            one = lax.rem(lax.div(index, bit), 2)
            other = lax.rem(lax.div(mask, bit), 2)
            result = result + bit * (one + other - 2 * one * other)
        bit *= 2
    return result


def farthest_first(index, i, size):
    if size % 2 or size & (size - 1):
        return partner(index, size - 1 - i, size)
    pair, core = lax.div(index, 2), lax.rem(index, 2)
    mask, odd = (size - 1 - i) // 2, lax.rem(i, 2)
    other = 1 - core
    odd = jnp.where(mask == 0, jnp.where(odd == 0, other, core), odd)
    return 2 * partner(pair, mask, size // 2) + odd


def nearest_first(index, i, size):
    if size % 2 or size & (size - 1) or size < 4:
        return partner(index, i, size)
    pair, core = lax.div(index, 2), lax.rem(index, 2)
    pairs = size // 2
    mask = jnp.where(i < 2, 0, 1 + lax.rem(i + pairs - 3, pairs - 1))
    odd = jnp.where(i < 2, jnp.where(i == 0, core, 1 - core), jnp.where(i < pairs + 1, 1, 0))
    return 2 * partner(pair, mask, pairs) + odd


def slot_of(source, target, size):
    return lax.rem(source - target - 1 + size, size)


def wait_bytes(ref, sem):
    pltpu.make_async_copy(ref, ref, sem).wait()


def project_one(vec, split, f, inverse, stage, at):
    rank, wide = vec.shape
    blocks = wide // 2
    lanes = lax.broadcasted_iota(jnp.int32, (1, wide), 1)
    high_minus = jnp.where(lanes < blocks, 1.0, -1.0).astype(jnp.float32)
    left = jnp.concatenate([high_minus * vec, pltpu.roll(vec, blocks, 1)], axis=0)
    high = left.astype(jnp.bfloat16)
    rest = (left - high.astype(jnp.float32)).astype(jnp.bfloat16)
    both = jnp.concatenate([high, high], axis=1)
    tail = jnp.concatenate([rest, jnp.zeros_like(rest)], axis=1)
    left = jnp.concatenate([both, tail], axis=0)
    for c in range(split.shape[1]):
        out = jnp.dot(left, split[f, c], preferred_element_type=jnp.float32)
        out = (out[: 2 * rank] + out[2 * rank :]) * inverse
        stage[at, 0, c] = out[:rank]
        stage[at, 1, c] = out[rank:]


def orthonormalize(z, turned, blocks, group):
    rank, wide = z.shape
    which = lax.broadcasted_iota(jnp.int32, (rank, wide), 0)
    for first in range(0, rank, group):
        rows = range(first, min(first + group, rank))
        real, imag = {}, {}
        for j in rows:
            real[j] = jnp.sum(z * z[j : j + 1], axis=1, keepdims=True)
            imag[j] = jnp.sum(z * turned[j : j + 1], axis=1, keepdims=True)
        for j in rows:
            real[j] = jnp.broadcast_to(real[j], z.shape) * (1.0 / blocks)
            imag[j] = jnp.broadcast_to(imag[j], z.shape) * (1.0 / blocks)
        for j in rows:
            square = jnp.maximum(real[j][j : j + 1], 0.0)
            factor = lax.rsqrt(square + EPS)
            gain = factor * factor
            gain = gain * (1.0 + EPS * gain)
            later = which > j
            along = jnp.where(later, real[j], 0.0)
            across = jnp.where(later, imag[j], 0.0)
            for k in rows:
                if k > j:
                    up = along[k : k + 1] * gain
                    side = across[k : k + 1] * gain
                    real[k] = real[k] - (up * along + side * across)
                    imag[k] = imag[k] - (up * across - side * along)
            unit = z[j : j + 1] * factor
            unit_turned = turned[j : j + 1] * factor
            along = along * factor
            across = across * factor
            z_next = z - (along * unit + across * unit_turned)
            turned = turned - (along * unit_turned - across * unit)
            z = jnp.where(which == j, unit, z_next)
    return z


def spod_kernel(
    scaling,
    freqs,
    peers,
    groups,
    early,
    data_ref,
    weight_hbm,
    basis_hbm,
    message_ref,
    energy_ref,
    trace_ref,
    inverse_ref,
    split,
    stage,
    buf,
    weight_ref,
    basis_ref,
    raw,
    gram_out,
    gram_in,
    trace_out,
    trace_in,
    message,
    energy_out,
    energy_in,
    small_sem,
    load_sem,
    gram_sem,
    trace_sem,
    msg_send,
    msg_recv,
    energy_sem,
    group_sem,
):
    comps, blocks, points = buf.shape[2], buf.shape[3], buf.shape[4]
    rank = basis_ref.shape[1]
    wide = 2 * blocks
    half_rows = blocks // 2
    stride = peers // freqs
    me = lax.axis_index("pts")
    row = lax.axis_index("freq")
    mine = lax.div(me, stride)
    is_owner = lax.rem(me, stride) == 0
    everyone = groups * peers
    hold = min(HOLD, freqs - 1)
    f32 = jnp.float32

    def load(f):
        return pltpu.make_async_copy(data_ref.at[:, f], buf.at[f], load_sem.at[f])

    def anyone(step):
        across, along = step // peers, step % peers
        return {"freq": partner(row, across, groups), "pts": partner(me, along, peers)}

    def order(i):
        return farthest_first(mine, i, freqs)

    weight_load = pltpu.make_async_copy(weight_hbm, weight_ref, small_sem.at[0])
    basis_load = pltpu.make_async_copy(basis_hbm.at[:, mine], basis_ref, small_sem.at[1])
    weight_load.start()
    for i in range(freqs):
        load(order(i)).start()
    basis_load.start()

    barrier = pltpu.get_barrier_semaphore()
    for step in range(1, peers):
        pl.semaphore_signal(
            barrier, inc=1, device_id={"pts": partner(me, step, peers)}, device_id_type=MESH
        )
    for step in range(1, groups):
        pl.semaphore_signal(
            barrier, inc=1, device_id={"freq": partner(row, step, groups)}, device_id_type=MESH
        )

    lanes = lax.broadcasted_iota(jnp.int32, (1, wide), 1)
    low = lanes < blocks
    high_minus = jnp.where(low, 1.0, -1.0).astype(f32)
    raw[...] = jnp.zeros_like(raw)
    weight_load.wait()
    root = jnp.sqrt(weight_ref[...])
    inverse = (1.0 / blocks) / root
    inverse_ref[...] = inverse

    rows_at = lax.broadcasted_iota(jnp.int32, (half_rows, wide), 0)
    cols_at = lax.broadcasted_iota(jnp.int32, (half_rows, wide), 1)
    diagonal = jnp.logical_or(cols_at == rows_at, cols_at == rows_at + blocks + half_rows)

    def local_gram(f):
        for c in range(comps):
            for part in range(2):
                value = buf[f, part, c] * root
                high = value.astype(jnp.bfloat16)
                rest = (value - high.astype(f32)).astype(jnp.bfloat16)
                split[f, c, part * blocks : (part + 1) * blocks] = high
                split[f, c, wide + part * blocks : wide + (part + 1) * blocks] = rest
        total = jnp.zeros((2 * wide, wide), f32)
        for c in range(comps):
            total = total + lax.dot_general(
                split[f, c],
                split[f, c, :wide],
                (((1,), (1,)), ((), ())),
                preferred_element_type=f32,
            )
        raw[...] = 0.5 * total[:wide] + total[wide:]

    def pack(f):
        total = raw[...]
        both = total[:blocks] + high_minus * pltpu.roll(total[blocks:], blocks, 1)
        other = pltpu.roll(both, blocks, 1)
        minus = both - other
        flipped = jnp.concatenate([minus, minus], axis=0).T
        full = both + other + flipped[:blocks]
        folded = jnp.where(low, full[:half_rows], full[half_rows:])
        gram_out[f] = folded
        return jnp.where(diagonal, folded, 0.0)

    def gram_copy(f):
        target = f * stride
        return pltpu.make_async_remote_copy(
            src_ref=gram_out.at[f],
            dst_ref=gram_in.at[slot_of(me, target, peers)],
            send_sem=gram_sem.at[0],
            recv_sem=gram_sem.at[1],
            device_id={"pts": target},
            device_id_type=MESH,
        )

    def opening(i, trace):
        load(order(i)).wait()
        trace = trace + pack(order(jnp.maximum(i - 1, 0)))
        local_gram(order(i))
        return trace

    trace = lax.fori_loop(0, hold, opening, jnp.zeros((half_rows, wide), f32))
    pl.semaphore_wait(barrier, peers - 1 + groups - 1)
    for step in range(1, groups):
        pl.semaphore_signal(
            group_sem, inc=1, device_id={"freq": partner(row, step, groups)}, device_id_type=MESH
        )
    for i in range(hold - 1):
        gram_copy(order(i)).start()

    def middle(i, trace):
        last = order(i - 1)
        load(order(i)).wait()
        trace = trace + pack(last)
        local_gram(order(i))
        gram_copy(last).start()
        return trace

    trace = lax.fori_loop(hold, freqs, middle, trace)
    trace = trace + pack(mine)
    if stride > 1:

        @pl.when(jnp.logical_not(is_owner))
        def _():
            gram_copy(mine).start()

    trace_row = jnp.sum(trace, axis=0, keepdims=True) * scaling
    trace_out[...] = trace_row

    def trace_copy(step):
        target = anyone(step)
        slot = slot_of(row * peers + me, target["freq"] * peers + target["pts"], everyone)
        return pltpu.make_async_remote_copy(
            src_ref=trace_out,
            dst_ref=trace_in.at[slot],
            send_sem=trace_sem.at[0],
            recv_sem=trace_sem.at[1],
            device_id=target,
            device_id_type=MESH,
        )

    pl.semaphore_wait(group_sem, groups - 1)
    for step in range(everyone - 1, 0, -1):
        trace_copy(step).start()

    def msg_copy(step):
        return pltpu.make_async_remote_copy(
            src_ref=message.at[mine],
            dst_ref=message.at[mine],
            send_sem=msg_send.at[0],
            recv_sem=msg_recv.at[mine],
            device_id={"pts": partner(me, step, peers)},
            device_id_type=MESH,
        )

    def energy_copy(step):
        target = partner(me, step, peers)
        return pltpu.make_async_remote_copy(
            src_ref=energy_out,
            dst_ref=energy_in.at[slot_of(mine, lax.div(target, stride), freqs)],
            send_sem=energy_sem.at[0],
            recv_sem=energy_sem.at[1],
            device_id={"pts": target},
            device_id_type=MESH,
        )

    basis_load.wait()

    @pl.when(is_owner)
    def _():
        wait_bytes(gram_in.at[pl.ds(0, peers - 1)], gram_sem.at[1])
        total = gram_out[mine]
        for k in range(peers - 1):
            total = total + gram_in[k]
        total = total * (0.5 * scaling)
        swapped = pltpu.roll(total, blocks, 1)
        full = jnp.concatenate(
            [jnp.where(low, total, swapped), jnp.where(low, swapped, total)], axis=0
        )
        full = jnp.concatenate([full, full], axis=0)
        flipped = full.T
        real = full + flipped
        imag = full - flipped
        top = lax.broadcasted_iota(jnp.int32, (wide, wide), 0) < blocks
        left = lax.broadcasted_iota(jnp.int32, (wide, wide), 1) < blocks
        same = top == left
        matrix = jnp.where(same, real, jnp.where(top, -imag, imag))
        turning = jnp.where(same, imag, jnp.where(top, real, -real))
        right = jnp.concatenate([matrix, turning], axis=1)

        def rounded(x):
            return x.astype(jnp.bfloat16).astype(f32)

        right_high = rounded(right)
        right_rest = right - right_high
        right_mid = rounded(right_rest)
        right_low = rounded(right_rest - right_mid)
        right_pair = jnp.concatenate([right_high, right_mid], axis=0)

        def apply(vec):
            high = rounded(vec)
            rest = vec - high
            mid = rounded(rest)
            tail = rounded(rest - mid)
            rows = jnp.concatenate(
                [
                    jnp.concatenate([high, high], axis=1),
                    jnp.concatenate([mid, mid], axis=1),
                    jnp.concatenate([tail, jnp.zeros_like(tail)], axis=1),
                ],
                axis=0,
            )
            out = jnp.dot(rows, right_pair, preferred_element_type=f32)
            small = jnp.dot(high, right_low, preferred_element_type=f32)
            out = out[:rank] + (out[rank : 2 * rank] + (out[2 * rank :] + small))
            return out[:, :wide], out[:, wide:]

        vec = jnp.concatenate([basis_ref[0], basis_ref[1]], axis=1)
        for step in range(ITERS):
            z, turned = apply(vec)
            vec = orthonormalize(z, turned, blocks, rank if step < ITERS - 1 else rank // 2)
        message[mine] = vec
        for step in range(peers - 1, 0, -1):
            msg_copy(step).start()
        energy = jnp.sum(vec * apply(vec)[0], axis=1, keepdims=True) * (1.0 / blocks)
        which = lax.broadcasted_iota(jnp.int32, (rank, wide), 0)
        columns = lax.broadcasted_iota(jnp.int32, (rank, wide), 1)
        energy_out[...] = jnp.sum(jnp.where(which == columns, energy, 0.0), axis=0, keepdims=True)
        for step in range(peers - 1, 0, -1):
            energy_copy(step).start()

    def arrive(i):
        f = nearest_first(mine, i, freqs)
        if stride > 1:

            @pl.when(jnp.logical_or(i > 0, jnp.logical_not(is_owner)))
            def _():
                wait_bytes(message.at[f], msg_recv.at[f])
        else:

            @pl.when(i > 0)
            def _():
                wait_bytes(message.at[f], msg_recv.at[f])

        return f

    def ahead(i, carry):
        f = arrive(i)
        project_one(message[f], split, f, inverse, stage, f)
        return carry

    lax.fori_loop(0, early, ahead, 0)
    for i in range(early, freqs):
        arrive(i)
    wait_bytes(trace_in.at[pl.ds(0, everyone - 1)], trace_sem.at[1])
    trace_ref[pl.ds(0, everyone - 1)] = trace_in[pl.ds(0, everyone - 1)]
    trace_ref[everyone - 1] = trace_out[...]
    if stride > 1:

        @pl.when(jnp.logical_not(is_owner))
        def _():
            wait_bytes(energy_in, energy_sem.at[1])
            energy_ref[...] = energy_in[...]

    @pl.when(is_owner)
    def _():
        wait_bytes(energy_in.at[pl.ds(0, freqs - 1)], energy_sem.at[1])
        energy_ref[pl.ds(0, freqs - 1)] = energy_in[pl.ds(0, freqs - 1)]
        energy_ref[freqs - 1] = energy_out[...]

    message_ref[...] = message[...]

    if stride > 1:

        @pl.when(jnp.logical_not(is_owner))
        def _():
            wait_bytes(gram_out, gram_sem.at[0])

        @pl.when(is_owner)
        def _():
            wait_bytes(gram_out.at[pl.ds(0, freqs - 1)], gram_sem.at[0])
    else:
        wait_bytes(gram_out.at[pl.ds(0, freqs - 1)], gram_sem.at[0])

    wait_bytes(trace_in.at[pl.ds(0, everyone - 1)], trace_sem.at[0])

    @pl.when(is_owner)
    def _():
        wait_bytes(trace_in.at[pl.ds(0, peers - 1)], energy_sem.at[0])
        wait_bytes(gram_in.at[pl.ds(0, peers - 1), pl.ds(0, rank)], msg_send.at[0])


def store_kernel(
    count,
    peers,
    early,
    message,
    energy,
    trace,
    inverse_ref,
    split,
    stage,
    basis_out,
    spectrum_out,
    modes_out,
    late_stage,
    basis_stage,
    spectrum_stage,
    store_sem,
):
    freqs, rank, wide = message.shape
    blocks = wide // 2
    mine = lax.div(lax.axis_index("pts"), peers // freqs)

    for i in range(early):
        f = nearest_first(mine, i, freqs)
        pltpu.make_async_copy(stage.at[f], modes_out.at[:, f], store_sem.at[0]).start()
    for i in range(early, freqs):
        f = nearest_first(mine, i, freqs)
        project_one(message[f], split, f, inverse_ref[...], late_stage, i - early)
        pltpu.make_async_copy(
            late_stage.at[i - early], modes_out.at[:, f], store_sem.at[0]
        ).start()

    vecs = message[...]
    turned = pltpu.roll(vecs, blocks, 2)
    basis_stage[0] = vecs[:, :, :blocks]
    basis_stage[1] = turned[:, :, :blocks]
    basis_store = pltpu.make_async_copy(basis_stage, basis_out, store_sem.at[1])
    basis_store.start()

    energies = jnp.concatenate(
        [energy[slot_of(f, mine, freqs)] for f in range(freqs)], axis=0
    )
    overall = jnp.sum(jnp.sum(trace[...], axis=0), axis=1, keepdims=True)
    spectrum = energies * count / overall
    spectrum_stage[...] = spectrum[:, :rank]
    spectrum_store = pltpu.make_async_copy(spectrum_stage, spectrum_out, store_sem.at[2])
    spectrum_store.start()

    wait_bytes(modes_out, store_sem.at[0])
    basis_store.wait()
    spectrum_store.wait()


def per_device(peers, groups, data, quad_weight, basis):
    _, freqs, blocks, comps, points = data.shape
    rank = basis.shape[-1]
    assert peers % freqs == 0 and freqs > 2
    scaling = 1.0 / (comps * points * peers)
    wide = 2 * blocks
    everyone = groups * peers
    early = freqs - LATE
    vmem = pl.BlockSpec(memory_space=pltpu.VMEM)
    anywhere = pl.BlockSpec(memory_space=pl.ANY)
    f32 = jnp.float32
    weight = quad_weight.reshape(1, points)
    hbm = pl.BlockSpec(memory_space=pltpu.HBM)
    in_hbm = functools.partial(pltpu.with_memory_space_constraint, memory_space=pltpu.HBM)
    message, energy, trace, inverse, split, stage = pl.pallas_call(
        functools.partial(spod_kernel, scaling, freqs, peers, groups, early),
        out_shape=(
            pltpu.VMEM((freqs, rank, wide), f32),
            pltpu.VMEM((freqs, 1, wide), f32),
            pltpu.VMEM((everyone, 1, wide), f32),
            pltpu.VMEM((1, points), f32),
            pltpu.VMEM((freqs, comps, 2 * wide, points), jnp.bfloat16),
            pltpu.VMEM((freqs, 2, comps, rank, points), f32),
        ),
        in_specs=[hbm, hbm, hbm],
        out_specs=(vmem, vmem, vmem, vmem, vmem, vmem),
        scratch_shapes=[
            pltpu.VMEM((freqs, 2, comps, blocks, points), f32),
            pltpu.VMEM((1, points), f32),
            pltpu.VMEM((2, rank, blocks), f32),
            pltpu.VMEM((wide, wide), f32),
            pltpu.VMEM((freqs, blocks // 2, wide), f32),
            pltpu.VMEM((peers, blocks // 2, wide), f32),
            pltpu.VMEM((1, wide), f32),
            pltpu.VMEM((everyone, 1, wide), f32),
            pltpu.VMEM((freqs, rank, wide), f32),
            pltpu.VMEM((1, wide), f32),
            pltpu.VMEM((freqs, 1, wide), f32),
            pltpu.SemaphoreType.DMA((2,)),
            pltpu.SemaphoreType.DMA((freqs,)),
            pltpu.SemaphoreType.DMA((2,)),
            pltpu.SemaphoreType.DMA((2,)),
            pltpu.SemaphoreType.DMA((1,)),
            pltpu.SemaphoreType.DMA((freqs,)),
            pltpu.SemaphoreType.DMA((2,)),
            pltpu.SemaphoreType.REGULAR,
        ],
        compiler_params=pltpu.CompilerParams(
            collective_id=0, has_side_effects=True, vmem_limit_bytes=44 * 1024 * 1024
        ),
        name="spod",
    )(
        in_hbm(data.transpose(0, 1, 3, 2, 4)),
        in_hbm(weight),
        in_hbm(basis.transpose(0, 1, 3, 2)),
    )
    basis_t, spectrum, modes_t = pl.pallas_call(
        functools.partial(store_kernel, freqs * groups * blocks, peers, early),
        out_shape=(
            jax.ShapeDtypeStruct((2, freqs, rank, blocks), f32),
            jax.ShapeDtypeStruct((freqs, rank), f32),
            jax.ShapeDtypeStruct((2, freqs, comps, rank, points), f32),
        ),
        in_specs=[vmem, vmem, vmem, vmem, vmem, vmem],
        out_specs=(anywhere, anywhere, anywhere),
        scratch_shapes=[
            pltpu.VMEM((freqs - early, 2, comps, rank, points), f32),
            pltpu.VMEM((2, freqs, rank, blocks), f32),
            pltpu.VMEM((freqs, rank), f32),
            pltpu.SemaphoreType.DMA((3,)),
        ],
        compiler_params=pltpu.CompilerParams(vmem_limit_bytes=20 * 1024 * 1024),
        name="store",
    )(message, energy, trace, inverse, split, stage)
    return (
        basis_t.transpose(0, 1, 3, 2),
        spectrum,
        modes_t.transpose(0, 1, 3, 2, 4),
    )


def solution(mesh):
    in_specs = (P(None, "freq", None, None, "pts"), P("pts"), P(None, "freq", None, None))
    out_specs = (P(None, "freq", None, None), P("freq", None), P(None, "freq", None, None, "pts"))
    body = functools.partial(per_device, mesh.shape["pts"], mesh.shape["freq"])
    return jax.shard_map(
        body, mesh=mesh, in_specs=in_specs, out_specs=out_specs, check_vma=False
    )
```

```python
import functools

import jax
import jax.numpy as jnp
from jax import lax
from jax.experimental import pallas as pl
from jax.experimental.pallas import tpu as pltpu
from jax.sharding import PartitionSpec as P

ITERS = 4
EPS = 1e-06
HOLD = 2
LATE = 2
MESH = pl.DeviceIdType.MESH


def partner(index, mask, size):
    if size & (size - 1):
        return lax.rem(index + mask, size)
    result, bit = 0, 1
    while bit < size:
        if isinstance(mask, int):
            one = lax.rem(lax.div(index, bit), 2)
            result = result + bit * (1 - one if mask & bit else one)
        else:
            one = lax.rem(lax.div(index, bit), 2)
            other = lax.rem(lax.div(mask, bit), 2)
            result = result + bit * (one + other - 2 * one * other)
        bit *= 2
    return result


def farthest_first(index, i, size):
    if size % 2 or size & (size - 1):
        return partner(index, size - 1 - i, size)
    pair, core = lax.div(index, 2), lax.rem(index, 2)
    mask, odd = (size - 1 - i) // 2, lax.rem(i, 2)
    other = 1 - core
    odd = jnp.where(mask == 0, jnp.where(odd == 0, other, core), odd)
    return 2 * partner(pair, mask, size // 2) + odd


def nearest_first(index, i, size):
    if size % 2 or size & (size - 1):
        return partner(index, i, size)
    pair, core = lax.div(index, 2), lax.rem(index, 2)
    mask, even = i // 2 if isinstance(i, int) else lax.div(i, 2), lax.rem(i, 2)
    odd = jnp.where(mask == 0, jnp.where(even == 0, core, 1 - core), 1 - even)
    return 2 * partner(pair, mask, size // 2) + odd


def slot_of(source, target, size):
    return lax.rem(source - target - 1 + size, size)


def wait_bytes(ref, sem):
    pltpu.make_async_copy(ref, ref, sem).wait()


def project_one(vec, split, f, inverse, stage, at):
    rank, wide = vec.shape
    blocks = wide // 2
    lanes = lax.broadcasted_iota(jnp.int32, (1, wide), 1)
    high_minus = jnp.where(lanes < blocks, 1.0, -1.0).astype(jnp.float32)
    left = jnp.concatenate([high_minus * vec, pltpu.roll(vec, blocks, 1)], axis=0)
    high = left.astype(jnp.bfloat16)
    rest = (left - high.astype(jnp.float32)).astype(jnp.bfloat16)
    both = jnp.concatenate([high, high], axis=1)
    tail = jnp.concatenate([rest, jnp.zeros_like(rest)], axis=1)
    left = jnp.concatenate([both, tail], axis=0)
    for c in range(split.shape[1]):
        out = jnp.dot(left, split[f, c], preferred_element_type=jnp.float32)
        out = (out[: 2 * rank] + out[2 * rank :]) * inverse
        stage[at, 0, c] = out[:rank]
        stage[at, 1, c] = out[rank:]


def orthonormalize(z, turned, blocks, group):
    rank, wide = z.shape
    which = lax.broadcasted_iota(jnp.int32, (rank, wide), 0)
    for first in range(0, rank, group):
        rows = range(first, min(first + group, rank))
        real, imag = {}, {}
        for j in rows:
            real[j] = jnp.sum(z * z[j : j + 1], axis=1, keepdims=True)
            imag[j] = jnp.sum(z * turned[j : j + 1], axis=1, keepdims=True)
        for j in rows:
            real[j] = jnp.broadcast_to(real[j], z.shape) * (1.0 / blocks)
            imag[j] = jnp.broadcast_to(imag[j], z.shape) * (1.0 / blocks)
        for j in rows:
            square = jnp.maximum(real[j][j : j + 1], 0.0)
            factor = lax.rsqrt(square + EPS)
            gain = factor * factor
            gain = gain * (1.0 + EPS * gain)
            later = which > j
            along = jnp.where(later, real[j], 0.0)
            across = jnp.where(later, imag[j], 0.0)
            for k in rows:
                if k > j:
                    up, side = along[k : k + 1], across[k : k + 1]
                    real[k] = real[k] - gain * (up * along + side * across)
                    imag[k] = imag[k] - gain * (up * across - side * along)
            unit = z[j : j + 1] * factor
            unit_turned = turned[j : j + 1] * factor
            along = along * factor
            across = across * factor
            z_next = z - (along * unit + across * unit_turned)
            turned = turned - (along * unit_turned - across * unit)
            z = jnp.where(which == j, unit, z_next)
    return z


def spod_kernel(
    scaling,
    freqs,
    peers,
    groups,
    early,
    data_ref,
    weight_hbm,
    basis_hbm,
    message_ref,
    energy_ref,
    trace_ref,
    inverse_ref,
    split,
    stage,
    buf,
    weight_ref,
    basis_ref,
    raw,
    gram_out,
    gram_in,
    trace_out,
    trace_in,
    message,
    energy_out,
    energy_in,
    small_sem,
    load_sem,
    gram_sem,
    trace_sem,
    msg_send,
    msg_recv,
    energy_sem,
    group_sem,
):
    comps, blocks, points = buf.shape[2], buf.shape[3], buf.shape[4]
    rank = basis_ref.shape[1]
    wide = 2 * blocks
    half_rows = blocks // 2
    stride = peers // freqs
    me = lax.axis_index("pts")
    row = lax.axis_index("freq")
    mine = lax.div(me, stride)
    is_owner = lax.rem(me, stride) == 0
    everyone = groups * peers
    hold = min(HOLD, freqs - 1)
    f32 = jnp.float32

    def load(f):
        return pltpu.make_async_copy(data_ref.at[:, f], buf.at[f], load_sem.at[f])

    def anyone(step):
        across, along = lax.div(step, peers), lax.rem(step, peers)
        return {"freq": partner(row, across, groups), "pts": partner(me, along, peers)}

    def order(i):
        return farthest_first(mine, i, freqs)

    weight_load = pltpu.make_async_copy(weight_hbm, weight_ref, small_sem.at[0])
    basis_load = pltpu.make_async_copy(basis_hbm.at[:, mine], basis_ref, small_sem.at[1])
    weight_load.start()
    for i in range(freqs):
        load(order(i)).start()
    basis_load.start()

    barrier = pltpu.get_barrier_semaphore()
    for step in range(1, peers):
        pl.semaphore_signal(
            barrier, inc=1, device_id={"pts": partner(me, step, peers)}, device_id_type=MESH
        )
    for step in range(1, groups):
        pl.semaphore_signal(
            barrier, inc=1, device_id={"freq": partner(row, step, groups)}, device_id_type=MESH
        )

    lanes = lax.broadcasted_iota(jnp.int32, (1, wide), 1)
    low = lanes < blocks
    high_minus = jnp.where(low, 1.0, -1.0).astype(f32)
    raw[...] = jnp.zeros_like(raw)
    weight_load.wait()
    root = jnp.sqrt(weight_ref[...])
    inverse = (1.0 / blocks) / root
    inverse_ref[...] = inverse

    rows_at = lax.broadcasted_iota(jnp.int32, (half_rows, wide), 0)
    cols_at = lax.broadcasted_iota(jnp.int32, (half_rows, wide), 1)
    diagonal = jnp.logical_or(cols_at == rows_at, cols_at == rows_at + blocks + half_rows)

    def local_gram(f):
        for c in range(comps):
            for part in range(2):
                value = buf[f, part, c] * root
                high = value.astype(jnp.bfloat16)
                rest = (value - high.astype(f32)).astype(jnp.bfloat16)
                split[f, c, part * blocks : (part + 1) * blocks] = high
                split[f, c, wide + part * blocks : wide + (part + 1) * blocks] = rest
        total = jnp.zeros((2 * wide, wide), f32)
        for c in range(comps):
            total = total + lax.dot_general(
                split[f, c],
                split[f, c, :wide],
                (((1,), (1,)), ((), ())),
                preferred_element_type=f32,
            )
        raw[...] = 0.5 * total[:wide] + total[wide:]

    def pack(f):
        total = raw[...]
        both = total[:blocks] + high_minus * pltpu.roll(total[blocks:], blocks, 1)
        other = pltpu.roll(both, blocks, 1)
        minus = both - other
        flipped = jnp.concatenate([minus, minus], axis=0).T
        full = both + other + flipped[:blocks]
        folded = jnp.where(low, full[:half_rows], full[half_rows:])
        gram_out[f] = folded
        return jnp.where(diagonal, folded, 0.0)

    def gram_copy(f):
        target = f * stride
        return pltpu.make_async_remote_copy(
            src_ref=gram_out.at[f],
            dst_ref=gram_in.at[slot_of(me, target, peers)],
            send_sem=gram_sem.at[0],
            recv_sem=gram_sem.at[1],
            device_id={"pts": target},
            device_id_type=MESH,
        )

    def opening(i, trace):
        load(order(i)).wait()
        trace = trace + pack(order(jnp.maximum(i - 1, 0)))
        local_gram(order(i))
        return trace

    trace = lax.fori_loop(0, hold, opening, jnp.zeros((half_rows, wide), f32))
    pl.semaphore_wait(barrier, peers - 1 + groups - 1)
    for step in range(1, groups):
        pl.semaphore_signal(
            group_sem, inc=1, device_id={"freq": partner(row, step, groups)}, device_id_type=MESH
        )
    for i in range(hold - 1):
        gram_copy(order(i)).start()

    def middle(i, trace):
        last = order(i - 1)
        load(order(i)).wait()
        trace = trace + pack(last)
        local_gram(order(i))
        gram_copy(last).start()
        return trace

    trace = lax.fori_loop(hold, freqs, middle, trace)
    trace = trace + pack(mine)
    if stride > 1:

        @pl.when(jnp.logical_not(is_owner))
        def _():
            gram_copy(mine).start()

    trace_row = jnp.sum(trace, axis=0, keepdims=True) * scaling
    trace_out[...] = trace_row

    def trace_copy(step):
        target = anyone(step)
        slot = slot_of(row * peers + me, target["freq"] * peers + target["pts"], everyone)
        return pltpu.make_async_remote_copy(
            src_ref=trace_out,
            dst_ref=trace_in.at[slot],
            send_sem=trace_sem.at[0],
            recv_sem=trace_sem.at[1],
            device_id=target,
            device_id_type=MESH,
        )

    pl.semaphore_wait(group_sem, groups - 1)
    def tell(step, carry):
        trace_copy(everyone - step).start()
        return carry

    lax.fori_loop(1, everyone, tell, 0)

    def msg_copy(step):
        return pltpu.make_async_remote_copy(
            src_ref=message.at[mine],
            dst_ref=message.at[mine],
            send_sem=msg_send.at[0],
            recv_sem=msg_recv.at[mine],
            device_id={"pts": partner(me, step, peers)},
            device_id_type=MESH,
        )

    def energy_copy(step):
        target = partner(me, step, peers)
        return pltpu.make_async_remote_copy(
            src_ref=energy_out,
            dst_ref=energy_in.at[slot_of(mine, lax.div(target, stride), freqs)],
            send_sem=energy_sem.at[0],
            recv_sem=energy_sem.at[1],
            device_id={"pts": target},
            device_id_type=MESH,
        )

    basis_load.wait()

    @pl.when(is_owner)
    def _():
        wait_bytes(gram_in.at[pl.ds(0, peers - 1)], gram_sem.at[1])
        total = gram_out[mine]
        for k in range(peers - 1):
            total = total + gram_in[k]
        total = total * (0.5 * scaling)
        swapped = pltpu.roll(total, blocks, 1)
        full = jnp.concatenate(
            [jnp.where(low, total, swapped), jnp.where(low, swapped, total)], axis=0
        )
        full = jnp.concatenate([full, full], axis=0)
        flipped = full.T
        real = full + flipped
        imag = full - flipped
        top = lax.broadcasted_iota(jnp.int32, (wide, wide), 0) < blocks
        left = lax.broadcasted_iota(jnp.int32, (wide, wide), 1) < blocks
        same = top == left
        matrix = jnp.where(same, real, jnp.where(top, -imag, imag))
        turning = jnp.where(same, imag, jnp.where(top, real, -real))
        right = jnp.concatenate([matrix, turning], axis=1)

        def rounded(x):
            return x.astype(jnp.bfloat16).astype(f32)

        right_high = rounded(right)
        right_rest = right - right_high
        right_mid = rounded(right_rest)
        right_low = rounded(right_rest - right_mid)
        right_pair = jnp.concatenate([right_high, right_mid], axis=0)

        def apply(vec):
            high = rounded(vec)
            rest = vec - high
            mid = rounded(rest)
            tail = rounded(rest - mid)
            rows = jnp.concatenate(
                [
                    jnp.concatenate([high, high], axis=1),
                    jnp.concatenate([mid, mid], axis=1),
                    jnp.concatenate([tail, jnp.zeros_like(tail)], axis=1),
                ],
                axis=0,
            )
            out = jnp.dot(rows, right_pair, preferred_element_type=f32)
            small = jnp.dot(high, right_low, preferred_element_type=f32)
            out = out[:rank] + (out[rank : 2 * rank] + (out[2 * rank :] + small))
            return out[:, :wide], out[:, wide:]

        vec = jnp.concatenate([basis_ref[0], basis_ref[1]], axis=1)
        for step in range(ITERS):
            z, turned = apply(vec)
            vec = orthonormalize(z, turned, blocks, rank if step < ITERS - 1 else rank // 2)
        message[mine] = vec
        for step in range(peers - 1, 0, -1):
            msg_copy(step).start()
        energy = jnp.sum(vec * apply(vec)[0], axis=1, keepdims=True) * (1.0 / blocks)
        which = lax.broadcasted_iota(jnp.int32, (rank, wide), 0)
        columns = lax.broadcasted_iota(jnp.int32, (rank, wide), 1)
        energy_out[...] = jnp.sum(jnp.where(which == columns, energy, 0.0), axis=0, keepdims=True)

        def tell_energy(step, carry):
            energy_copy(peers - step).start()
            return carry

        lax.fori_loop(1, peers, tell_energy, 0)

    def arrive(i):
        f = nearest_first(mine, i, freqs)
        if stride > 1:

            @pl.when(jnp.logical_or(i > 0, jnp.logical_not(is_owner)))
            def _():
                wait_bytes(message.at[f], msg_recv.at[f])
        else:

            @pl.when(i > 0)
            def _():
                wait_bytes(message.at[f], msg_recv.at[f])

        return f

    def ahead(k, carry):
        fs = [arrive(2 * k), arrive(2 * k + 1)]
        for f in fs:
            project_one(message[f], split, f, inverse, stage, f)
        return carry

    lax.fori_loop(0, early // 2, ahead, 0)
    if early % 2:
        f = arrive(early - 1)
        project_one(message[f], split, f, inverse, stage, f)
    for i in range(early, freqs):
        arrive(i)
    wait_bytes(trace_in.at[pl.ds(0, everyone - 1)], trace_sem.at[1])
    trace_ref[pl.ds(0, everyone - 1)] = trace_in[pl.ds(0, everyone - 1)]
    trace_ref[everyone - 1] = trace_out[...]
    if stride > 1:

        @pl.when(jnp.logical_not(is_owner))
        def _():
            wait_bytes(energy_in, energy_sem.at[1])
            energy_ref[...] = energy_in[...]

    @pl.when(is_owner)
    def _():
        wait_bytes(energy_in.at[pl.ds(0, freqs - 1)], energy_sem.at[1])
        energy_ref[pl.ds(0, freqs - 1)] = energy_in[pl.ds(0, freqs - 1)]
        energy_ref[freqs - 1] = energy_out[...]

    message_ref[...] = message[...]

    if stride > 1:

        @pl.when(jnp.logical_not(is_owner))
        def _():
            wait_bytes(gram_out, gram_sem.at[0])

        @pl.when(is_owner)
        def _():
            wait_bytes(gram_out.at[pl.ds(0, freqs - 1)], gram_sem.at[0])
    else:
        wait_bytes(gram_out.at[pl.ds(0, freqs - 1)], gram_sem.at[0])

    wait_bytes(trace_in.at[pl.ds(0, everyone - 1)], trace_sem.at[0])

    @pl.when(is_owner)
    def _():
        wait_bytes(trace_in.at[pl.ds(0, peers - 1)], energy_sem.at[0])
        wait_bytes(gram_in.at[pl.ds(0, peers - 1), pl.ds(0, rank)], msg_send.at[0])


def store_kernel(
    count,
    peers,
    early,
    message,
    energy,
    trace,
    inverse_ref,
    split,
    stage,
    basis_out,
    spectrum_out,
    modes_out,
    late_stage,
    basis_stage,
    spectrum_stage,
    store_sem,
):
    freqs, rank, wide = message.shape
    blocks = wide // 2
    mine = lax.div(lax.axis_index("pts"), peers // freqs)

    for i in range(early):
        f = nearest_first(mine, i, freqs)
        pltpu.make_async_copy(stage.at[f], modes_out.at[:, f], store_sem.at[0]).start()
    for i in range(early, freqs):
        f = nearest_first(mine, i, freqs)
        project_one(message[f], split, f, inverse_ref[...], late_stage, i - early)
        pltpu.make_async_copy(
            late_stage.at[i - early], modes_out.at[:, f], store_sem.at[0]
        ).start()

    vecs = message[...]
    turned = pltpu.roll(vecs, blocks, 2)
    basis_stage[0] = vecs[:, :, :blocks]
    basis_stage[1] = turned[:, :, :blocks]
    basis_store = pltpu.make_async_copy(basis_stage, basis_out, store_sem.at[1])
    basis_store.start()

    energies = jnp.concatenate(
        [energy[slot_of(f, mine, freqs)] for f in range(freqs)], axis=0
    )
    overall = jnp.sum(jnp.sum(trace[...], axis=0), axis=1, keepdims=True)
    spectrum = energies * count / overall
    spectrum_stage[...] = spectrum[:, :rank]
    spectrum_store = pltpu.make_async_copy(spectrum_stage, spectrum_out, store_sem.at[2])
    spectrum_store.start()

    wait_bytes(modes_out, store_sem.at[0])
    basis_store.wait()
    spectrum_store.wait()


def per_device(peers, groups, data, quad_weight, basis):
    _, freqs, blocks, comps, points = data.shape
    rank = basis.shape[-1]
    assert peers % freqs == 0 and freqs > 2
    scaling = 1.0 / (comps * points * peers)
    wide = 2 * blocks
    everyone = groups * peers
    early = freqs - LATE
    vmem = pl.BlockSpec(memory_space=pltpu.VMEM)
    anywhere = pl.BlockSpec(memory_space=pl.ANY)
    f32 = jnp.float32
    weight = quad_weight.reshape(1, points)
    hbm = pl.BlockSpec(memory_space=pltpu.HBM)
    in_hbm = functools.partial(pltpu.with_memory_space_constraint, memory_space=pltpu.HBM)
    message, energy, trace, inverse, split, stage = pl.pallas_call(
        functools.partial(spod_kernel, scaling, freqs, peers, groups, early),
        out_shape=(
            pltpu.VMEM((freqs, rank, wide), f32),
            pltpu.VMEM((freqs, 1, wide), f32),
            pltpu.VMEM((everyone, 1, wide), f32),
            pltpu.VMEM((1, points), f32),
            pltpu.VMEM((freqs, comps, 2 * wide, points), jnp.bfloat16),
            pltpu.VMEM((freqs, 2, comps, rank, points), f32),
        ),
        in_specs=[hbm, hbm, hbm],
        out_specs=(vmem, vmem, vmem, vmem, vmem, vmem),
        scratch_shapes=[
            pltpu.VMEM((freqs, 2, comps, blocks, points), f32),
            pltpu.VMEM((1, points), f32),
            pltpu.VMEM((2, rank, blocks), f32),
            pltpu.VMEM((wide, wide), f32),
            pltpu.VMEM((freqs, blocks // 2, wide), f32),
            pltpu.VMEM((peers, blocks // 2, wide), f32),
            pltpu.VMEM((1, wide), f32),
            pltpu.VMEM((everyone, 1, wide), f32),
            pltpu.VMEM((freqs, rank, wide), f32),
            pltpu.VMEM((1, wide), f32),
            pltpu.VMEM((freqs, 1, wide), f32),
            pltpu.SemaphoreType.DMA((2,)),
            pltpu.SemaphoreType.DMA((freqs,)),
            pltpu.SemaphoreType.DMA((2,)),
            pltpu.SemaphoreType.DMA((2,)),
            pltpu.SemaphoreType.DMA((1,)),
            pltpu.SemaphoreType.DMA((freqs,)),
            pltpu.SemaphoreType.DMA((2,)),
            pltpu.SemaphoreType.REGULAR,
        ],
        compiler_params=pltpu.CompilerParams(
            collective_id=0, has_side_effects=True, vmem_limit_bytes=44 * 1024 * 1024
        ),
        name="spod",
    )(
        in_hbm(data.transpose(0, 1, 3, 2, 4)),
        in_hbm(weight),
        in_hbm(basis.transpose(0, 1, 3, 2)),
    )
    basis_t, spectrum, modes_t = pl.pallas_call(
        functools.partial(store_kernel, freqs * groups * blocks, peers, early),
        out_shape=(
            jax.ShapeDtypeStruct((2, freqs, rank, blocks), f32),
            jax.ShapeDtypeStruct((freqs, rank), f32),
            jax.ShapeDtypeStruct((2, freqs, comps, rank, points), f32),
        ),
        in_specs=[vmem, vmem, vmem, vmem, vmem, vmem],
        out_specs=(anywhere, anywhere, anywhere),
        scratch_shapes=[
            pltpu.VMEM((freqs - early, 2, comps, rank, points), f32),
            pltpu.VMEM((2, freqs, rank, blocks), f32),
            pltpu.VMEM((freqs, rank), f32),
            pltpu.SemaphoreType.DMA((3,)),
        ],
        compiler_params=pltpu.CompilerParams(vmem_limit_bytes=20 * 1024 * 1024),
        name="store",
    )(message, energy, trace, inverse, split, stage)
    return (
        basis_t.transpose(0, 1, 3, 2),
        spectrum,
        modes_t.transpose(0, 1, 3, 2, 4),
    )


def solution(mesh):
    in_specs = (P(None, "freq", None, None, "pts"), P("pts"), P(None, "freq", None, None))
    out_specs = (P(None, "freq", None, None), P("freq", None), P(None, "freq", None, None, "pts"))
    body = functools.partial(per_device, mesh.shape["pts"], mesh.shape["freq"])
    return jax.shard_map(
        body, mesh=mesh, in_specs=in_specs, out_specs=out_specs, check_vma=False
    )
```

```python
import functools

import jax
import jax.numpy as jnp
from jax import lax
from jax.experimental import pallas as pl
from jax.experimental.pallas import tpu as pltpu
from jax.sharding import PartitionSpec as P

ITERS = 4
EPS = 1e-06
HOLD = 2
LATE = 2
MESH = pl.DeviceIdType.MESH


def partner(index, mask, size):
    if size & (size - 1):
        return lax.rem(index + mask, size)
    result, bit = 0, 1
    while bit < size:
        if isinstance(mask, int):
            one = lax.rem(lax.div(index, bit), 2)
            result = result + bit * (1 - one if mask & bit else one)
        else:
            one = lax.rem(lax.div(index, bit), 2)
            other = lax.rem(lax.div(mask, bit), 2)
            result = result + bit * (one + other - 2 * one * other)
        bit *= 2
    return result


def farthest_first(index, i, size):
    if size % 2 or size & (size - 1):
        return partner(index, size - 1 - i, size)
    pair, core = lax.div(index, 2), lax.rem(index, 2)
    mask, odd = (size - 1 - i) // 2, lax.rem(i, 2)
    other = 1 - core
    odd = jnp.where(mask == 0, jnp.where(odd == 0, other, core), odd)
    return 2 * partner(pair, mask, size // 2) + odd


def nearest_first(index, i, size):
    if size % 2 or size & (size - 1):
        return partner(index, i, size)
    pair, core = lax.div(index, 2), lax.rem(index, 2)
    mask, even = i // 2 if isinstance(i, int) else lax.div(i, 2), lax.rem(i, 2)
    odd = jnp.where(mask == 0, jnp.where(even == 0, core, 1 - core), 1 - even)
    return 2 * partner(pair, mask, size // 2) + odd


def slot_of(source, target, size):
    return lax.rem(source - target - 1 + size, size)


def wait_bytes(ref, sem):
    pltpu.make_async_copy(ref, ref, sem).wait()


def project_one(vec, split, f, inverse, stage, at):
    rank, wide = vec.shape
    blocks = wide // 2
    lanes = lax.broadcasted_iota(jnp.int32, (1, wide), 1)
    high_minus = jnp.where(lanes < blocks, 1.0, -1.0).astype(jnp.float32)
    left = jnp.concatenate([high_minus * vec, pltpu.roll(vec, blocks, 1)], axis=0)
    high = left.astype(jnp.bfloat16)
    rest = (left - high.astype(jnp.float32)).astype(jnp.bfloat16)
    both = jnp.concatenate([high, high], axis=1)
    tail = jnp.concatenate([rest, jnp.zeros_like(rest)], axis=1)
    left = jnp.concatenate([both, tail], axis=0)
    for c in range(split.shape[1]):
        out = jnp.dot(left, split[f, c], preferred_element_type=jnp.float32)
        out = (out[: 2 * rank] + out[2 * rank :]) * inverse
        stage[at, 0, c] = out[:rank]
        stage[at, 1, c] = out[rank:]


def orthonormalize(z, turned, blocks, group):
    rank, wide = z.shape
    which = lax.broadcasted_iota(jnp.int32, (rank, wide), 0)
    for first in range(0, rank, group):
        rows = range(first, min(first + group, rank))
        real, imag = {}, {}
        for j in rows:
            real[j] = jnp.sum(z * z[j : j + 1], axis=1, keepdims=True)
            imag[j] = jnp.sum(z * turned[j : j + 1], axis=1, keepdims=True)
        for j in rows:
            real[j] = jnp.broadcast_to(real[j], z.shape) * (1.0 / blocks)
            imag[j] = jnp.broadcast_to(imag[j], z.shape) * (1.0 / blocks)
        for j in rows:
            square = jnp.maximum(real[j][j : j + 1], 0.0)
            factor = lax.rsqrt(square + EPS)
            gain = factor * factor
            gain = gain * (1.0 + EPS * gain)
            later = which > j
            along = jnp.where(later, real[j], 0.0)
            across = jnp.where(later, imag[j], 0.0)
            for k in rows:
                if k > j:
                    up, side = along[k : k + 1], across[k : k + 1]
                    real[k] = real[k] - gain * (up * along + side * across)
                    imag[k] = imag[k] - gain * (up * across - side * along)
            unit = z[j : j + 1] * factor
            unit_turned = turned[j : j + 1] * factor
            along = along * factor
            across = across * factor
            z_next = z - (along * unit + across * unit_turned)
            turned = turned - (along * unit_turned - across * unit)
            z = jnp.where(which == j, unit, z_next)
    return z


def spod_kernel(
    scaling,
    freqs,
    peers,
    groups,
    early,
    data_ref,
    weight_hbm,
    basis_hbm,
    message_ref,
    energy_ref,
    trace_ref,
    inverse_ref,
    split,
    stage,
    buf,
    weight_ref,
    basis_ref,
    raw,
    gram_out,
    gram_in,
    trace_out,
    trace_in,
    message,
    energy_out,
    energy_in,
    small_sem,
    load_sem,
    gram_sem,
    trace_sem,
    msg_send,
    msg_recv,
    energy_sem,
    group_sem,
):
    comps, blocks, points = buf.shape[2], buf.shape[3], buf.shape[4]
    rank = basis_ref.shape[1]
    wide = 2 * blocks
    half_rows = blocks // 2
    stride = peers // freqs
    me = lax.axis_index("pts")
    row = lax.axis_index("freq")
    mine = lax.div(me, stride)
    is_owner = lax.rem(me, stride) == 0
    everyone = groups * peers
    hold = min(HOLD, freqs - 1)
    f32 = jnp.float32

    def load(f):
        return pltpu.make_async_copy(data_ref.at[:, f], buf.at[f], load_sem.at[f])

    def anyone(step):
        across, along = lax.div(step, peers), lax.rem(step, peers)
        return {"freq": partner(row, across, groups), "pts": partner(me, along, peers)}

    def order(i):
        return farthest_first(mine, i, freqs)

    weight_load = pltpu.make_async_copy(weight_hbm, weight_ref, small_sem.at[0])
    basis_load = pltpu.make_async_copy(basis_hbm.at[:, mine], basis_ref, small_sem.at[1])
    weight_load.start()
    for i in range(freqs):
        load(order(i)).start()
    basis_load.start()

    barrier = pltpu.get_barrier_semaphore()
    for step in range(1, peers):
        pl.semaphore_signal(
            barrier, inc=1, device_id={"pts": partner(me, step, peers)}, device_id_type=MESH
        )
    for step in range(1, groups):
        pl.semaphore_signal(
            barrier, inc=1, device_id={"freq": partner(row, step, groups)}, device_id_type=MESH
        )

    lanes = lax.broadcasted_iota(jnp.int32, (1, wide), 1)
    low = lanes < blocks
    high_minus = jnp.where(low, 1.0, -1.0).astype(f32)
    raw[...] = jnp.zeros_like(raw)
    weight_load.wait()
    root = jnp.sqrt(weight_ref[...])
    inverse = (1.0 / blocks) / root
    inverse_ref[...] = inverse

    rows_at = lax.broadcasted_iota(jnp.int32, (half_rows, wide), 0)
    cols_at = lax.broadcasted_iota(jnp.int32, (half_rows, wide), 1)
    diagonal = jnp.logical_or(cols_at == rows_at, cols_at == rows_at + blocks + half_rows)

    def times(left, right):
        return lax.dot_general(left, right, (((1,), (1,)), ((), ())), preferred_element_type=f32)

    def local_gram(f):
        for c in range(comps):
            for part in range(2):
                value = buf[f, part, c] * root
                high = value.astype(jnp.bfloat16)
                rest = (value - high.astype(f32)).astype(jnp.bfloat16)
                split[f, c, part * blocks : (part + 1) * blocks] = high
                split[f, c, wide + part * blocks : wide + (part + 1) * blocks] = rest
        tall = jnp.zeros((2 * wide, wide), f32)
        broad = jnp.zeros((wide, 2 * wide), f32)
        chunk = points // 2
        for k in range(2 * comps):
            at = pl.ds((k % 2) * chunk, chunk)
            whole, high = split[f, k // 2, :, at], split[f, k // 2, :wide, at]
            if k in (0, 1, 4):
                tall = tall + times(whole, high)
            else:
                broad = broad + times(high, whole)
        raw[...] = 0.5 * (tall[:wide] + broad[:, :wide]) + (tall[wide:] + broad[:, wide:])

    def pack(f):
        total = raw[...]
        both = total[:blocks] + high_minus * pltpu.roll(total[blocks:], blocks, 1)
        other = pltpu.roll(both, blocks, 1)
        minus = both - other
        flipped = jnp.concatenate([minus, minus], axis=0).T
        full = both + other + flipped[:blocks]
        folded = jnp.where(low, full[:half_rows], full[half_rows:])
        gram_out[f] = folded
        return jnp.where(diagonal, folded, 0.0)

    def gram_copy(f):
        target = f * stride
        return pltpu.make_async_remote_copy(
            src_ref=gram_out.at[f],
            dst_ref=gram_in.at[slot_of(me, target, peers)],
            send_sem=gram_sem.at[0],
            recv_sem=gram_sem.at[1],
            device_id={"pts": target},
            device_id_type=MESH,
        )

    def opening(i, trace):
        load(order(i)).wait()
        trace = trace + pack(order(jnp.maximum(i - 1, 0)))
        local_gram(order(i))
        return trace

    trace = lax.fori_loop(0, hold, opening, jnp.zeros((half_rows, wide), f32))
    pl.semaphore_wait(barrier, peers - 1 + groups - 1)
    for step in range(1, groups):
        pl.semaphore_signal(
            group_sem, inc=1, device_id={"freq": partner(row, step, groups)}, device_id_type=MESH
        )
    for i in range(hold - 1):
        gram_copy(order(i)).start()

    def middle(i, trace):
        last = order(i - 1)
        load(order(i)).wait()
        trace = trace + pack(last)
        local_gram(order(i))
        gram_copy(last).start()
        return trace

    trace = lax.fori_loop(hold, freqs, middle, trace)
    trace = trace + pack(mine)
    if stride > 1:

        @pl.when(jnp.logical_not(is_owner))
        def _():
            gram_copy(mine).start()

    trace_row = jnp.sum(trace, axis=0, keepdims=True) * scaling
    trace_out[...] = trace_row

    def trace_copy(step):
        target = anyone(step)
        slot = slot_of(row * peers + me, target["freq"] * peers + target["pts"], everyone)
        return pltpu.make_async_remote_copy(
            src_ref=trace_out,
            dst_ref=trace_in.at[slot],
            send_sem=trace_sem.at[0],
            recv_sem=trace_sem.at[1],
            device_id=target,
            device_id_type=MESH,
        )

    pl.semaphore_wait(group_sem, groups - 1)
    def tell(step, carry):
        trace_copy(everyone - step).start()
        return carry

    lax.fori_loop(1, everyone, tell, 0)

    def msg_copy(step):
        return pltpu.make_async_remote_copy(
            src_ref=message.at[mine],
            dst_ref=message.at[mine],
            send_sem=msg_send.at[0],
            recv_sem=msg_recv.at[mine],
            device_id={"pts": partner(me, step, peers)},
            device_id_type=MESH,
        )

    def energy_copy(step):
        target = partner(me, step, peers)
        return pltpu.make_async_remote_copy(
            src_ref=energy_out,
            dst_ref=energy_in.at[slot_of(mine, lax.div(target, stride), freqs)],
            send_sem=energy_sem.at[0],
            recv_sem=energy_sem.at[1],
            device_id={"pts": target},
            device_id_type=MESH,
        )

    basis_load.wait()

    @pl.when(is_owner)
    def _():
        wait_bytes(gram_in.at[pl.ds(0, peers - 1)], gram_sem.at[1])
        total = gram_out[mine]
        for k in range(peers - 1):
            total = total + gram_in[k]
        total = total * (0.5 * scaling)
        swapped = pltpu.roll(total, blocks, 1)
        full = jnp.concatenate(
            [jnp.where(low, total, swapped), jnp.where(low, swapped, total)], axis=0
        )
        full = jnp.concatenate([full, full], axis=0)
        flipped = full.T
        real = full + flipped
        imag = full - flipped
        top = lax.broadcasted_iota(jnp.int32, (wide, wide), 0) < blocks
        left = lax.broadcasted_iota(jnp.int32, (wide, wide), 1) < blocks
        same = top == left
        matrix = jnp.where(same, real, jnp.where(top, -imag, imag))
        turning = jnp.where(same, imag, jnp.where(top, real, -real))
        right = jnp.concatenate([matrix, turning], axis=1)

        def rounded(x):
            return x.astype(jnp.bfloat16).astype(f32)

        right_high = rounded(right)
        right_rest = right - right_high
        right_mid = rounded(right_rest)
        right_low = rounded(right_rest - right_mid)
        right_pair = jnp.concatenate([right_high, right_mid], axis=0)

        def apply(vec):
            high = rounded(vec)
            rest = vec - high
            mid = rounded(rest)
            tail = rounded(rest - mid)
            rows = jnp.concatenate(
                [
                    jnp.concatenate([high, high], axis=1),
                    jnp.concatenate([mid, mid], axis=1),
                    jnp.concatenate([tail, jnp.zeros_like(tail)], axis=1),
                ],
                axis=0,
            )
            out = jnp.dot(rows, right_pair, preferred_element_type=f32)
            small = jnp.dot(high, right_low, preferred_element_type=f32)
            out = out[:rank] + (out[rank : 2 * rank] + (out[2 * rank :] + small))
            return out[:, :wide], out[:, wide:]

        vec = jnp.concatenate([basis_ref[0], basis_ref[1]], axis=1)
        for step in range(ITERS):
            z, turned = apply(vec)
            vec = orthonormalize(z, turned, blocks, rank if step < ITERS - 1 else rank // 2)
        message[mine] = vec
        for step in range(peers - 1, 0, -1):
            msg_copy(step).start()
        energy = jnp.sum(vec * apply(vec)[0], axis=1, keepdims=True) * (1.0 / blocks)
        which = lax.broadcasted_iota(jnp.int32, (rank, wide), 0)
        columns = lax.broadcasted_iota(jnp.int32, (rank, wide), 1)
        energy_out[...] = jnp.sum(jnp.where(which == columns, energy, 0.0), axis=0, keepdims=True)

        def tell_energy(step, carry):
            energy_copy(peers - step).start()
            return carry

        lax.fori_loop(1, peers, tell_energy, 0)

    def arrive(i):
        f = nearest_first(mine, i, freqs)
        if stride > 1:

            @pl.when(jnp.logical_or(i > 0, jnp.logical_not(is_owner)))
            def _():
                wait_bytes(message.at[f], msg_recv.at[f])
        else:

            @pl.when(i > 0)
            def _():
                wait_bytes(message.at[f], msg_recv.at[f])

        return f

    def ahead(k, carry):
        fs = [arrive(2 * k), arrive(2 * k + 1)]
        for f in fs:
            project_one(message[f], split, f, inverse, stage, f)
        return carry

    lax.fori_loop(0, early // 2, ahead, 0)
    if early % 2:
        f = arrive(early - 1)
        project_one(message[f], split, f, inverse, stage, f)
    for i in range(early, freqs):
        arrive(i)
    wait_bytes(trace_in.at[pl.ds(0, everyone - 1)], trace_sem.at[1])
    trace_ref[pl.ds(0, everyone - 1)] = trace_in[pl.ds(0, everyone - 1)]
    trace_ref[everyone - 1] = trace_out[...]
    if stride > 1:

        @pl.when(jnp.logical_not(is_owner))
        def _():
            wait_bytes(energy_in, energy_sem.at[1])
            energy_ref[...] = energy_in[...]

    @pl.when(is_owner)
    def _():
        wait_bytes(energy_in.at[pl.ds(0, freqs - 1)], energy_sem.at[1])
        energy_ref[pl.ds(0, freqs - 1)] = energy_in[pl.ds(0, freqs - 1)]
        energy_ref[freqs - 1] = energy_out[...]

    message_ref[...] = message[...]

    if stride > 1:

        @pl.when(jnp.logical_not(is_owner))
        def _():
            wait_bytes(gram_out, gram_sem.at[0])

        @pl.when(is_owner)
        def _():
            wait_bytes(gram_out.at[pl.ds(0, freqs - 1)], gram_sem.at[0])
    else:
        wait_bytes(gram_out.at[pl.ds(0, freqs - 1)], gram_sem.at[0])

    wait_bytes(trace_in.at[pl.ds(0, everyone - 1)], trace_sem.at[0])

    @pl.when(is_owner)
    def _():
        wait_bytes(trace_in.at[pl.ds(0, peers - 1)], energy_sem.at[0])
        wait_bytes(gram_in.at[pl.ds(0, peers - 1), pl.ds(0, rank)], msg_send.at[0])


def store_kernel(
    count,
    peers,
    early,
    message,
    energy,
    trace,
    inverse_ref,
    split,
    stage,
    basis_out,
    spectrum_out,
    modes_out,
    late_stage,
    basis_stage,
    spectrum_stage,
    store_sem,
):
    freqs, rank, wide = message.shape
    blocks = wide // 2
    mine = lax.div(lax.axis_index("pts"), peers // freqs)

    for i in range(early):
        f = nearest_first(mine, i, freqs)
        pltpu.make_async_copy(stage.at[f], modes_out.at[:, f], store_sem.at[0]).start()
    for i in range(early, freqs):
        f = nearest_first(mine, i, freqs)
        project_one(message[f], split, f, inverse_ref[...], late_stage, i - early)
        pltpu.make_async_copy(
            late_stage.at[i - early], modes_out.at[:, f], store_sem.at[0]
        ).start()

    vecs = message[...]
    turned = pltpu.roll(vecs, blocks, 2)
    basis_stage[0] = vecs[:, :, :blocks]
    basis_stage[1] = turned[:, :, :blocks]
    basis_store = pltpu.make_async_copy(basis_stage, basis_out, store_sem.at[1])
    basis_store.start()

    energies = jnp.concatenate(
        [energy[slot_of(f, mine, freqs)] for f in range(freqs)], axis=0
    )
    overall = jnp.sum(jnp.sum(trace[...], axis=0), axis=1, keepdims=True)
    spectrum = energies * count / overall
    spectrum_stage[...] = spectrum[:, :rank]
    spectrum_store = pltpu.make_async_copy(spectrum_stage, spectrum_out, store_sem.at[2])
    spectrum_store.start()

    wait_bytes(modes_out, store_sem.at[0])
    basis_store.wait()
    spectrum_store.wait()


def per_device(peers, groups, data, quad_weight, basis):
    _, freqs, blocks, comps, points = data.shape
    rank = basis.shape[-1]
    assert peers % freqs == 0 and freqs > 2
    scaling = 1.0 / (comps * points * peers)
    wide = 2 * blocks
    everyone = groups * peers
    early = freqs - LATE
    vmem = pl.BlockSpec(memory_space=pltpu.VMEM)
    anywhere = pl.BlockSpec(memory_space=pl.ANY)
    f32 = jnp.float32
    weight = quad_weight.reshape(1, points)
    hbm = pl.BlockSpec(memory_space=pltpu.HBM)
    in_hbm = functools.partial(pltpu.with_memory_space_constraint, memory_space=pltpu.HBM)
    message, energy, trace, inverse, split, stage = pl.pallas_call(
        functools.partial(spod_kernel, scaling, freqs, peers, groups, early),
        out_shape=(
            pltpu.VMEM((freqs, rank, wide), f32),
            pltpu.VMEM((freqs, 1, wide), f32),
            pltpu.VMEM((everyone, 1, wide), f32),
            pltpu.VMEM((1, points), f32),
            pltpu.VMEM((freqs, comps, 2 * wide, points), jnp.bfloat16),
            pltpu.VMEM((freqs, 2, comps, rank, points), f32),
        ),
        in_specs=[hbm, hbm, hbm],
        out_specs=(vmem, vmem, vmem, vmem, vmem, vmem),
        scratch_shapes=[
            pltpu.VMEM((freqs, 2, comps, blocks, points), f32),
            pltpu.VMEM((1, points), f32),
            pltpu.VMEM((2, rank, blocks), f32),
            pltpu.VMEM((wide, wide), f32),
            pltpu.VMEM((freqs, blocks // 2, wide), f32),
            pltpu.VMEM((peers, blocks // 2, wide), f32),
            pltpu.VMEM((1, wide), f32),
            pltpu.VMEM((everyone, 1, wide), f32),
            pltpu.VMEM((freqs, rank, wide), f32),
            pltpu.VMEM((1, wide), f32),
            pltpu.VMEM((freqs, 1, wide), f32),
            pltpu.SemaphoreType.DMA((2,)),
            pltpu.SemaphoreType.DMA((freqs,)),
            pltpu.SemaphoreType.DMA((2,)),
            pltpu.SemaphoreType.DMA((2,)),
            pltpu.SemaphoreType.DMA((1,)),
            pltpu.SemaphoreType.DMA((freqs,)),
            pltpu.SemaphoreType.DMA((2,)),
            pltpu.SemaphoreType.REGULAR,
        ],
        compiler_params=pltpu.CompilerParams(
            collective_id=0, has_side_effects=True, vmem_limit_bytes=44 * 1024 * 1024
        ),
        name="spod",
    )(
        in_hbm(data.transpose(0, 1, 3, 2, 4)),
        in_hbm(weight),
        in_hbm(basis.transpose(0, 1, 3, 2)),
    )
    basis_t, spectrum, modes_t = pl.pallas_call(
        functools.partial(store_kernel, freqs * groups * blocks, peers, early),
        out_shape=(
            jax.ShapeDtypeStruct((2, freqs, rank, blocks), f32),
            jax.ShapeDtypeStruct((freqs, rank), f32),
            jax.ShapeDtypeStruct((2, freqs, comps, rank, points), f32),
        ),
        in_specs=[vmem, vmem, vmem, vmem, vmem, vmem],
        out_specs=(anywhere, anywhere, anywhere),
        scratch_shapes=[
            pltpu.VMEM((freqs - early, 2, comps, rank, points), f32),
            pltpu.VMEM((2, freqs, rank, blocks), f32),
            pltpu.VMEM((freqs, rank), f32),
            pltpu.SemaphoreType.DMA((3,)),
        ],
        compiler_params=pltpu.CompilerParams(vmem_limit_bytes=20 * 1024 * 1024),
        name="store",
    )(message, energy, trace, inverse, split, stage)
    return (
        basis_t.transpose(0, 1, 3, 2),
        spectrum,
        modes_t.transpose(0, 1, 3, 2, 4),
    )


def solution(mesh):
    in_specs = (P(None, "freq", None, None, "pts"), P("pts"), P(None, "freq", None, None))
    out_specs = (P(None, "freq", None, None), P("freq", None), P(None, "freq", None, None, "pts"))
    body = functools.partial(per_device, mesh.shape["pts"], mesh.shape["freq"])
    return jax.shard_map(
        body, mesh=mesh, in_specs=in_specs, out_specs=out_specs, check_vma=False
    )
```
